32 devices in a mesh: gz: 4 (over y, x), gy: 8 (over z, core).
Axes of the slice: x: 2, y: 2, z: 4, core: 2. Of those that a mesh axis runs over, the one named last changes fastest.
Arguments:
- grid_grad: float32 [64, 128, 512], P('gz', 'gy'), may hold values from -6 to 6
- cells: int32 [3, 65536], P(None, ('gz', 'gy')), may hold values from 0 to 511, as said below
- offsets: int32 [3, 65536], P(None, ('gz', 'gy')), may hold values from 0 to 1023
- owners: int32 [65536, 1], P(('gz', 'gy')), may hold values from 0 to 31; in each aligned block of 2048 rows (0 to 2047, 2048 to 4095, ...) at most 128 rows name the same one
- slots: int32 [65536], P(('gz', 'gy')), may hold values from 0 to 2047
Outputs:
- pos_grad: float32 [3, 65536], P(None, ('gz', 'gy'))
The draws below stay inside these ranges and needn't reach their ends.
Inputs may be any that keep to these rules, and one draw needn't show every extreme that they name: `cells`: the row's cell lies in the mesh block of the device that holds the row: along z in [gz * 16, gz * 16 + 16), along y in [gy * 16, gy * 16 + 16), where gz, gy are that device's indices. `owners`: owners are linear device indices gz * 8 + gy. Among the rows of one device, no owner is named by more than 128 rows; some owner is named by exactly 128.
All inputs are finite; a program needn't handle non-finite values.
Results may differ from the reference program's by a relative error of at most 0.0003.
Values sent between devices are 32-bit elements; how exact they have to be, the bound alone decides.
A program may use at most 64 MiB of HBM per device.

```python
import math
import jax
import jax.numpy as jnp
import numpy as np

CZ = 16
CY = 16
LX = 512
P_DEV = 2048
NZ = 64
NY = 128
PROWS = 65536
CAP = 128
N_GZ = 4
N_GY = 8
DEVICES = 32


def draw_cells(key, part):
    total_rows = P_DEV * N_GZ * N_GY
    device = jnp.arange(total_rows, dtype=jnp.int32) // P_DEV
    index_z = device // N_GY
    index_y = device % N_GY
    key_z = jax.random.fold_in(key, 11)
    key_y = jax.random.fold_in(key, 12)
    key_x = jax.random.fold_in(key, 13)
    cell_z = index_z * CZ + jax.random.randint(key_z, (total_rows,), 0, CZ, dtype=jnp.int32)
    cell_y = index_y * CY + jax.random.randint(key_y, (total_rows,), 0, CY, dtype=jnp.int32)
    cell_x = jax.random.randint(key_x, (total_rows,), 0, LX, dtype=jnp.int32)
    return jnp.stack([cell_z, cell_y, cell_x]).astype(jnp.int32)


def set_ends(result, rng, low, largest):
    extent = result.shape
    place = [jax.random.randint(jax.random.fold_in(rng, axis), (), 0, extent[axis]) for axis in range(len(extent))]
    result = result.at[tuple(place)].set(low)
    longest = extent.index(max(extent))
    place[longest] = (place[longest] + 1) % extent[longest]
    return result.at[tuple(place)].set(largest)


def levels(stream_key, shape, pieces, smallest, largest):
    def one(dim, shards_of):
        heights = jax.random.uniform(jax.random.fold_in(jax.random.fold_in(stream_key, 6), dim), (shards_of,), jnp.float32, smallest / len(pieces), largest / len(pieces))
        return jnp.repeat(jnp.exp(heights), shape[dim] // shards_of).reshape((-1,) + (1,) * (len(shape) - dim - 1))

    gain = one(*pieces[0])
    for cut in pieces[1:]:
        gain = gain * one(*cut)
    return gain


def shared_out(rng, own, number, rows, count, top, bound, lean):
    ranking = jax.random.permutation(rng, count)
    heavy_load, ordinary = load_shares(count, rows * top, bound, lean, True), load_shares(count, rows * top, bound, lean, False)
    places = jnp.arange(count)

    def named(sizes, rotation):
        used = int((sizes > 0).sum())
        fixed = max(1, used // 4)
        passed = fixed + (places - fixed + rotation * (used - fixed)) % max(1, count - fixed)
        return jnp.zeros((count,), jnp.int32).at[ranking[jnp.where(places < fixed, places, passed)]].set(jnp.asarray(sizes, jnp.int32))

    sizes = jnp.where(number % 4 == 0, named(heavy_load, number // 4), named(ordinary, number - number // 4 - 1))
    mixed = jax.random.permutation(jax.random.fold_in(own, 3), count)
    source_of, sink = mixed[0:count // 2 * 2:2], mixed[1:count // 2 * 2:2]
    room = jnp.minimum(sizes[source_of] - 1, bound - sizes[sink]) // 2
    room = jnp.where((source_of == ranking[0]) | (sink == ranking[0]) | (sizes[sink] == 0), 0, jnp.maximum(room, 0))
    passed = jax.random.randint(jax.random.fold_in(own, 4), (count // 2,), 0, 1 << 20) % (room + 1)
    sizes = sizes.at[source_of].add(-passed).at[sink].add(passed)
    members = jnp.searchsorted(jnp.cumsum(sizes), jnp.arange(rows * top), side="right").astype(jnp.int32)
    table = members.reshape(top, rows).T
    table = table[jax.random.permutation(jax.random.fold_in(own, 1), rows)]
    rotation = jax.random.randint(jax.random.fold_in(own, 2), (rows, 1), 0, top)
    return jnp.take_along_axis(table, (jnp.arange(top)[None, :] + rotation) % top, axis=1)


def load_shares(number_of, total, most, skew, full):
    loads = [(1 << 20) // math.isqrt(standing ** skew) + 1 for standing in range(1, number_of + 1)]
    largest = most if full else min(most, max(-(-total // number_of), total * loads[0] // sum(loads)))
    least = 1 if total - largest >= number_of - 1 else 0
    holding, surplus = [largest] + [least] * (number_of - 1), total - largest - least * (number_of - 1)
    while surplus > 0:
        free = [i for i in range(1, number_of) if holding[i] < largest] or [i for i in range(1, number_of) if holding[i] < most]
        pool, remaining = sum([loads[i] for i in free]), surplus
        for i in free:
            extra = min(most - holding[i], max(1, remaining * loads[i] // pool), surplus)
            holding[i] = holding[i] + extra
            surplus = surplus - extra
    return np.array(holding)


def scatter_about(stream_key, extent, spread, limit, pieces=(), kind=jnp.bfloat16):
    loudness = levels(stream_key, extent, pieces, -0.22, 0.18) if pieces else 1.0
    array = jax.random.normal(stream_key, extent, jnp.float32) * spread * loudness
    return jnp.minimum(jnp.maximum(array, -limit), limit).astype(kind)


def setup_inputs(seed: int = 0) -> dict:
    streams_of = jax.random.split(jax.random.key(seed), 6)
    grid_grad = scatter_about(streams_of[0], (NZ, NY, LX), 1.0, 6.0, ((0, 4), (1, 8)), jnp.float32)
    cells = draw_cells(jax.random.fold_in(streams_of[5], 71), 0)
    offsets = set_ends(jax.random.randint(streams_of[2], (3, PROWS), 0, 1024), jax.random.fold_in(streams_of[2], 1), 0, 1023).astype(jnp.int32)
    owners_keys = jax.random.split(jax.random.fold_in(streams_of[3], 1), PROWS // P_DEV)
    owners_turns = jax.random.permutation(jax.random.fold_in(streams_of[3], 3), PROWS // P_DEV)
    owners = jax.vmap(lambda own, number: shared_out(jax.random.fold_in(streams_of[3], 2), own, number, P_DEV, DEVICES, 1, CAP, 2))(owners_keys, owners_turns).reshape((PROWS, 1))
    slots = set_ends(jax.random.randint(streams_of[4], (PROWS,), 0, P_DEV), jax.random.fold_in(streams_of[4], 1), 0, P_DEV - 1).astype(jnp.int32)
    return {"grid_grad": grid_grad, "cells": cells, "offsets": offsets, "owners": owners, "slots": slots}


def cic_gradient(corner, fraction):
    weight_z = (1.0 - fraction[0], fraction[0])
    weight_y = (1.0 - fraction[1], fraction[1])
    weight_x = (1.0 - fraction[2], fraction[2])
    grad_z = jnp.zeros_like(fraction[0])
    grad_y = jnp.zeros_like(fraction[0])
    grad_x = jnp.zeros_like(fraction[0])
    for first in range(2):
        for second in range(2):
            grad_z = grad_z + (corner[1][first][second] - corner[0][first][second]) * weight_y[first] * weight_x[second]
            grad_y = grad_y + (corner[first][1][second] - corner[first][0][second]) * weight_z[first] * weight_x[second]
            grad_x = grad_x + (corner[first][second][1] - corner[first][second][0]) * weight_z[first] * weight_y[second]
    return jnp.stack([grad_z, grad_y, grad_x])


def reference(grid_grad, cells, offsets, owners, slots):
    size_z, size_y, size_x = grid_grad.shape
    fraction = (offsets.astype(jnp.float32) + 0.5) / 1024.0
    flat = grid_grad.reshape(-1)
    corner = []
    for step_z in range(2):
        plane = []
        for step_y in range(2):
            line = []
            for step_x in range(2):
                pos_z = (cells[0] + step_z) % size_z
                pos_y = (cells[1] + step_y) % size_y
                pos_x = (cells[2] + step_x) % size_x
                line.append(flat[(pos_z * size_y + pos_y) * size_x + pos_x])
            plane.append(line)
        corner.append(plane)
    gradient = cic_gradient(corner, fraction)
    target = (owners[:, 0] * P_DEV + slots).astype(jnp.int32)
    total = jnp.zeros((3, cells.shape[1]), jnp.float32)
    return total.at[:, target].add(gradient)
```

```python
import functools

import jax
import jax.numpy as jnp
from jax import lax
from jax.experimental import pallas as pl
from jax.experimental.pallas import tpu as pltpu
from jax.sharding import PartitionSpec as P

MESH = pl.DeviceIdType.MESH
BF = jnp.bfloat16
F32 = jnp.float32
LANES = 128


def iota(shape, axis):
    return lax.broadcasted_iota(jnp.int32, shape, axis)


def hot(mask):
    return jnp.where(mask, 1.0, 0.0).astype(BF)


def split(value):
    high = value.astype(BF)
    low = (value - high.astype(F32)).astype(BF)
    return high, low


def dot_nn(a, b):
    return lax.dot_general(a, b, (((1,), (0,)), ((), ())), preferred_element_type=F32)


def dot_nt(a, b):
    return lax.dot_general(a, b, (((1,), (1,)), ((), ())), preferred_element_type=F32)


def with_diff(rows):
    size_x = rows.shape[1]
    diff = pltpu.roll(rows, size_x - 1, 1) - rows
    return jnp.concatenate([*split(rows), *split(diff)], axis=0)


def over(count, step, carry):
    if count == 1:
        return step(0, carry)
    return lax.fori_loop(0, count, step, carry)


def kernel(
    grid_ref, cells, offsets, owners, slots, out,
    grid_v, row_s, corner_s, halo_z, halo_y, halo_c, mesh_s, hot_s, acc_s, rank_s, vals_s,
    send_s, recv_s, grid_sem, halo_send, halo_recv, all_send, all_recv,
):
    count_z, count_y = lax.axis_size("gz"), lax.axis_size("gy")
    devices = count_z * count_y
    gz, gy = lax.axis_index("gz"), lax.axis_index("gy")
    me = gz * count_y + gy
    size_z, size_y, size_x = grid_ref.shape
    rows = cells.shape[1]
    chunk = min(256, rows)
    chunks = rows // chunk
    group = min(32, devices)
    groups = devices // group
    slab = size_z * size_y

    load = pltpu.make_async_copy(grid_ref, grid_v, grid_sem)
    load.start()
    barrier = pltpu.get_barrier_semaphore()

    def coords(shift):
        other = lax.rem(me + shift, devices)
        return (other // count_y, lax.rem(other, count_y))

    def greet(shift, carry):
        pl.semaphore_signal(barrier, inc=1, device_id=coords(shift), device_id_type=MESH)
        return carry

    lax.fori_loop(1, devices, greet, 0)

    owner = owners[...]
    before = hot(iota((chunk, chunk), 0) < iota((chunk, chunk), 1))

    def rank_group(g, ranks):
        mine = jnp.where(iota((group, rows), 0) + g * group == owner, 1.0, 0.0)
        pieces = [mine[:, c * chunk:(c + 1) * chunk] for c in range(chunks)]
        inside = dot_nn(jnp.concatenate(pieces, axis=0).astype(BF), before)
        start = jnp.zeros((group, 1), F32)
        found = []
        for c in range(chunks):
            where = inside[c * group:(c + 1) * group] + start
            found.append(jnp.sum(pieces[c] * where, axis=0, keepdims=True))
            start = start + jnp.sum(pieces[c], axis=1, keepdims=True)
        return ranks + jnp.concatenate(found, axis=1)

    ranks = over(groups, rank_group, jnp.zeros((1, rows), F32))
    rank_s[...] = hot(iota((LANES, rows), 0) == ranks.astype(jnp.int32))

    load.wait()
    row_s[...] = grid_v[:, 0, :]
    corner_s[...] = grid_v[0, 0:1, :]
    mesh_s[...] = with_diff(grid_v[...].reshape(slab, size_x))

    pl.semaphore_wait(barrier, devices - 1)
    below_z = lax.rem(gz + count_z - 1, count_z)
    below_y = lax.rem(gy + count_y - 1, count_y)
    halos = []
    for i, (source, target, device) in enumerate((
        (grid_ref.at[0], halo_z, (below_z, gy)),
        (row_s, halo_y, (gz, below_y)),
        (corner_s, halo_c, (below_z, below_y)),
    )):
        halos.append(pltpu.make_async_remote_copy(
            src_ref=source, dst_ref=target, send_sem=halo_send.at[i], recv_sem=halo_recv.at[i],
            device_id=device, device_id_type=MESH,
        ))
        halos[-1].start()

    def place(j):
        span = pl.ds(pl.multiple_of(j * chunk, chunk), chunk)
        cell = cells[:, span]
        frac = (offsets[:, span].astype(F32) + 0.5) / 1024.0
        return (span, cell[0:1] - gz * size_z, cell[1:2] - gy * size_y, cell[2:3],
                frac[0:1], frac[1:2], frac[2:3])

    def main_chunk(j, carry):
        span, cz, cy, cx, fz, fy, fx = place(j)
        onehot = hot(iota((size_x, chunk), 0) == cx)
        hot_s[:, span] = onehot
        prod = dot_nn(mesh_s[...], onehot)
        shape = (size_y, chunk)
        cz, fz = jnp.broadcast_to(cz, shape), jnp.broadcast_to(fz, shape)
        gz0 = 1.0 - fz
        total = [jnp.zeros(shape, F32) for _ in range(4)]
        for z in range(size_z):
            lower, upper = cz == z, cz == z - 1
            weight = jnp.where(lower, gz0, jnp.where(upper, fz, 0.0))
            diff = jnp.where(lower, -1.0, jnp.where(upper, 1.0, 0.0))
            at = [prod[q * slab + z * size_y:q * slab + (z + 1) * size_y] for q in range(4)]
            value, slope = at[0] + at[1], at[2] + at[3]
            total[0] += weight * value
            total[1] += diff * value
            total[2] += weight * slope
            total[3] += diff * slope
        for q in range(4):
            acc_s[q, :, span] = total[q]
        return carry

    lax.fori_loop(0, chunks, main_chunk, 0)

    for copy in halos:
        copy.wait()
    ghost = jnp.concatenate(
        [halo_z[...], halo_y[...], jnp.broadcast_to(halo_c[...], (8, size_x))], axis=0)
    ghost = with_diff(ghost)
    part = size_y + size_z + 8

    def halo_chunk(j, carry):
        span, cz, cy, cx, fz, fy, fx = place(j)
        prod = dot_nn(ghost, hot_s[:, span])
        value = prod[:part] + prod[part:2 * part]
        slope = prod[2 * part:3 * part] + prod[3 * part:]
        top_z, top_y = cz == size_z - 1, cy == size_y - 1
        wz_top, dz_top = jnp.where(top_z, fz, 0.0), jnp.where(top_z, 1.0, 0.0)
        wy_top, dy_top = jnp.where(top_y, fy, 0.0), jnp.where(top_y, 1.0, 0.0)
        a_w = acc_s[0, :, span] + wz_top * value[:size_y]
        a_d = acc_s[1, :, span] + dz_top * value[:size_y]
        b_w = acc_s[2, :, span] + wz_top * slope[:size_y]
        b_d = acc_s[3, :, span] + dz_top * slope[:size_y]
        place_y = iota((size_y, chunk), 0)
        lower, upper = place_y == cy, place_y == cy + 1
        w_y = jnp.where(lower, 1.0 - fy, jnp.where(upper, fy, 0.0))
        d_y = jnp.where(lower, -1.0, jnp.where(upper, 1.0, 0.0))
        grad_z = jnp.sum((a_d + fx * b_d) * w_y, axis=0, keepdims=True)
        grad_y = jnp.sum((a_w + fx * b_w) * d_y, axis=0, keepdims=True)
        grad_x = jnp.sum(b_w * w_y, axis=0, keepdims=True)
        place_z = iota((size_z, chunk), 0)
        lower, upper = place_z == cz, place_z == cz + 1
        w_z = jnp.where(lower, 1.0 - fz, jnp.where(upper, fz, 0.0))
        d_z = jnp.where(lower, -1.0, jnp.where(upper, 1.0, 0.0))
        side = slice(size_y, size_y + size_z)
        corner = slice(size_y + size_z, size_y + size_z + 1)
        read = value[side] + fx * slope[side]
        read_c = value[corner] + fx * slope[corner]
        h_w = jnp.sum(read * w_z, axis=0, keepdims=True) + read_c * wz_top
        h_d = jnp.sum(read * d_z, axis=0, keepdims=True) + read_c * dz_top
        h_x = jnp.sum(slope[side] * w_z, axis=0, keepdims=True) + slope[corner] * wz_top
        record = (slots[:, span] + 1).astype(F32)
        vals_s[:, span] = jnp.concatenate(
            [grad_z + wy_top * h_d, grad_y + dy_top * h_w, grad_x + wy_top * h_x, record] * 2, axis=0)
        return carry

    lax.fori_loop(0, chunks, halo_chunk, 0)

    def pack_group(g, carry):
        wide = 4 * group
        whose = lax.shift_right_logical(iota((wide, rows), 0), 2) + g * group
        values = jnp.concatenate([vals_s[...]] * (wide // 8), axis=0)
        high, low = split(jnp.where(whose == owner, values, 0.0))
        packed = dot_nt(high, rank_s[...]) + dot_nt(low, rank_s[...])
        for d in range(group):
            send_s[g * group + d] = packed[4 * d:4 * d + 4]
        return carry

    over(groups, pack_group, 0)

    def exchange(source, target, device):
        return pltpu.make_async_remote_copy(
            src_ref=source, dst_ref=target, send_sem=all_send, recv_sem=all_recv,
            device_id=device, device_id_type=MESH,
        )

    def post(shift, carry):
        other = lax.rem(me + shift, devices)
        exchange(send_s.at[other], recv_s.at[me], coords(shift)).start()
        return carry

    lax.fori_loop(1, devices, post, 0)
    recv_s[me] = send_s[me]
    others = pl.ds(0, devices - 1)
    exchange(send_s.at[others], recv_s.at[others], coords(1)).wait()

    highs = rows // LANES

    def add_group(g, total):
        block = jnp.concatenate([recv_s[g * group + d] for d in range(group)], axis=1)
        record = block[3:4].astype(jnp.int32) - 1
        high_at = lax.shift_right_arithmetic(record, 7)
        low_at = lax.bitwise_and(record, LANES - 1)
        width = block.shape[1]
        low_hot = hot(iota((LANES, width), 0) == low_at)
        values = jnp.concatenate([block] * highs, axis=0)
        which = lax.shift_right_logical(iota((4 * highs, width), 0), 2)
        both = jnp.concatenate(split(jnp.where(which == high_at, values, 0.0)), axis=0)
        added = dot_nt(both, low_hot)
        return total + added[:4 * highs] + added[4 * highs:]

    total = over(groups, add_group, jnp.zeros((4 * highs, LANES), F32))
    for h in range(highs):
        out[:, h * LANES:(h + 1) * LANES] = total[4 * h:4 * h + 3]


def body(grid_grad, cells, offsets, owners, slots):
    size_z, size_y, size_x = grid_grad.shape
    rows = cells.shape[1]
    devices = lax.axis_size("gz") * lax.axis_size("gy")
    vmem = pl.BlockSpec(memory_space=pltpu.VMEM)
    part = size_y + size_z + 8
    return pl.pallas_call(
        kernel,
        out_shape=jax.ShapeDtypeStruct((3, rows), F32),
        in_specs=[pl.BlockSpec(memory_space=pl.ANY), vmem, vmem, vmem, vmem],
        out_specs=vmem,
        scratch_shapes=[
            pltpu.VMEM((size_z, size_y, size_x), F32),
            pltpu.VMEM((size_z, size_x), F32),
            pltpu.VMEM((1, size_x), F32),
            pltpu.VMEM((size_y, size_x), F32),
            pltpu.VMEM((size_z, size_x), F32),
            pltpu.VMEM((1, size_x), F32),
            pltpu.VMEM((4 * size_z * size_y, size_x), BF),
            pltpu.VMEM((size_x, rows), BF),
            pltpu.VMEM((4, size_y, rows), F32),
            pltpu.VMEM((LANES, rows), BF),
            pltpu.VMEM((8, rows), F32),
            pltpu.VMEM((devices, 4, LANES), F32),
            pltpu.VMEM((devices, 4, LANES), F32),
            pltpu.SemaphoreType.DMA,
            pltpu.SemaphoreType.DMA((3,)),
            pltpu.SemaphoreType.DMA((3,)),
            pltpu.SemaphoreType.DMA,
            pltpu.SemaphoreType.DMA,
        ],
        compiler_params=pltpu.CompilerParams(collective_id=0, has_side_effects=True),
        name="cic",
    )(grid_grad, cells, offsets, owners.reshape(1, rows), slots.reshape(1, rows))


def solution(mesh):
    placed = (
        P("gz", "gy", None),
        P(None, ("gz", "gy")),
        P(None, ("gz", "gy")),
        P(("gz", "gy"), None),
        P(("gz", "gy")),
    )
    return jax.shard_map(
        body, mesh=mesh, in_specs=placed, out_specs=P(None, ("gz", "gy")), check_vma=False
    )
```

```python
import jax
import jax.numpy as jnp
from jax import lax
from jax.experimental import pallas as pl
from jax.experimental.pallas import tpu as pltpu
from jax.sharding import PartitionSpec as P

MESH = pl.DeviceIdType.MESH
BF = jnp.bfloat16
F32 = jnp.float32
LANES = 128


def iota(shape, axis):
    return lax.broadcasted_iota(jnp.int32, shape, axis)


def hot(mask):
    return jnp.where(mask, 1.0, 0.0).astype(BF)


def split(value):
    high = value.astype(BF)
    low = (value - high.astype(F32)).astype(BF)
    return high, low


def dot_nn(a, b):
    return lax.dot_general(a, b, (((1,), (0,)), ((), ())), preferred_element_type=F32)


def dot_nt(a, b):
    return lax.dot_general(a, b, (((1,), (1,)), ((), ())), preferred_element_type=F32)


def with_diff(rows):
    size_x = rows.shape[1]
    diff = pltpu.roll(rows, size_x - 1, 1) - rows
    return jnp.concatenate([*split(rows), *split(diff)], axis=0)


def over(count, step, carry):
    if count == 1:
        return step(0, carry)
    return lax.fori_loop(0, count, step, carry)


def kernel(
    grid_ref, cells_ref, offsets_ref, owners_ref, slots_ref, out,
    cells, offsets, owners, slots, grid_v, row_s, corner_s, halo_z, halo_y, halo_c, mesh_s, hot_s, acc_s, rank_s, vals_s,
    send_s, recv_s, load_sem, halo_send, halo_recv, all_send, all_recv,
):
    count_z, count_y = lax.axis_size("gz"), lax.axis_size("gy")
    devices = count_z * count_y
    gz, gy = lax.axis_index("gz"), lax.axis_index("gy")
    me = gz * count_y + gy
    size_z, size_y, size_x = grid_ref.shape
    rows = cells.shape[1]
    chunk = min(256, rows)
    chunks = rows // chunk
    group = min(32, devices)
    groups = devices // group
    slab = size_z * size_y

    loads = []
    for i, (source, target) in enumerate((
        (owners_ref, owners), (grid_ref, grid_v), (cells_ref, cells),
        (offsets_ref, offsets), (slots_ref, slots),
    )):
        loads.append(pltpu.make_async_copy(source, target, load_sem.at[i]))
        loads[-1].start()
    barrier = pltpu.get_barrier_semaphore()

    def each_other(act):
        few = devices <= 64

        def along_y(to_z, first):
            def step(shift, carry):
                act(to_z, lax.rem(gy + shift, count_y))
                return carry
            lax.fori_loop(first, count_y, step, 0, unroll=few)

        along_y(gz, 1)

        def step_z(shift, carry):
            along_y(lax.rem(gz + shift, count_z), 0)
            return carry
        lax.fori_loop(1, count_z, step_z, 0, unroll=few)

    def greet(to_z, to_y):
        pl.semaphore_signal(barrier, inc=1, device_id=(to_z, to_y), device_id_type=MESH)

    each_other(greet)

    loads[0].wait()
    owner = owners[...]
    before = hot(iota((chunk, chunk), 0) < iota((chunk, chunk), 1))

    def rank_group(g, ranks):
        mine = jnp.where(iota((group, rows), 0) + g * group == owner, 1.0, 0.0)
        pieces = [mine[:, c * chunk:(c + 1) * chunk] for c in range(chunks)]
        inside = dot_nn(jnp.concatenate(pieces, axis=0).astype(BF), before)
        start = jnp.zeros((group, 1), F32)
        found = []
        for c in range(chunks):
            where = inside[c * group:(c + 1) * group] + start
            found.append(jnp.sum(pieces[c] * where, axis=0, keepdims=True))
            start = start + jnp.sum(pieces[c], axis=1, keepdims=True)
        return ranks + jnp.concatenate(found, axis=1)

    ranks = over(groups, rank_group, jnp.zeros((1, rows), F32))
    rank_s[...] = hot(iota((LANES, rows), 0) == ranks.astype(jnp.int32))

    loads[1].wait()
    row_s[...] = grid_v[:, 0, :]
    corner_s[...] = grid_v[0, 0:1, :]
    mesh_s[...] = with_diff(grid_v[...].reshape(slab, size_x))

    for copy in loads[2:]:
        copy.wait()

    def place(j):
        span = pl.ds(j * chunk, chunk)
        cell = cells[:, span]
        frac = (offsets[:, span].astype(F32) + 0.5) / 1024.0
        return (span, cell[0:1] - gz * size_z, cell[1:2] - gy * size_y, cell[2:3],
                frac[0:1], frac[1:2], frac[2:3])

    def main_chunk(j):
        span, cz, cy, cx, fz, fy, fx = place(j)
        onehot = hot(iota((size_x, chunk), 0) == cx)
        hot_s[:, span] = onehot
        prod = dot_nn(mesh_s[...], onehot)
        cz, fz = jnp.broadcast_to(cz, (8, chunk)), jnp.broadcast_to(fz, (8, chunk))
        gz0 = 1.0 - fz
        tiles = size_y // 8
        total = [[jnp.zeros((8, chunk), F32) for _ in range(tiles)] for _ in range(4)]
        for z in range(size_z):
            lower, upper = cz == z, cz == z - 1
            weight = jnp.where(lower, gz0, jnp.where(upper, fz, 0.0))
            diff = jnp.where(lower, -1.0, jnp.where(upper, 1.0, 0.0))
            for t in range(tiles):
                first = z * size_y + 8 * t
                at = [prod[q * slab + first:q * slab + first + 8] for q in range(4)]
                value, slope = at[0] + at[1], at[2] + at[3]
                total[0][t] += weight * value
                total[1][t] += diff * value
                total[2][t] += weight * slope
                total[3][t] += diff * slope
        for q in range(4):
            acc_s[q, :, span] = jnp.concatenate(total[q], axis=0)

    part = size_y + size_z + 8

    def halo_chunk(j, ghost):
        span, cz, cy, cx, fz, fy, fx = place(j)
        prod = dot_nn(ghost, hot_s[:, span])
        value = prod[:part] + prod[part:2 * part]
        slope = prod[2 * part:3 * part] + prod[3 * part:]
        top_z, top_y = cz == size_z - 1, cy == size_y - 1
        wz_top, dz_top = jnp.where(top_z, fz, 0.0), jnp.where(top_z, 1.0, 0.0)
        wy_top, dy_top = jnp.where(top_y, fy, 0.0), jnp.where(top_y, 1.0, 0.0)
        a_w = acc_s[0, :, span] + wz_top * value[:size_y]
        a_d = acc_s[1, :, span] + dz_top * value[:size_y]
        b_w = acc_s[2, :, span] + wz_top * slope[:size_y]
        b_d = acc_s[3, :, span] + dz_top * slope[:size_y]
        place_y = iota((size_y, chunk), 0)
        lower, upper = place_y == cy, place_y == cy + 1
        w_y = jnp.where(lower, 1.0 - fy, jnp.where(upper, fy, 0.0))
        d_y = jnp.where(lower, -1.0, jnp.where(upper, 1.0, 0.0))
        grad_z = jnp.sum((a_d + fx * b_d) * w_y, axis=0, keepdims=True)
        grad_y = jnp.sum((a_w + fx * b_w) * d_y, axis=0, keepdims=True)
        grad_x = jnp.sum(b_w * w_y, axis=0, keepdims=True)
        place_z = iota((size_z, chunk), 0)
        lower, upper = place_z == cz, place_z == cz + 1
        w_z = jnp.where(lower, 1.0 - fz, jnp.where(upper, fz, 0.0))
        d_z = jnp.where(lower, -1.0, jnp.where(upper, 1.0, 0.0))
        side = slice(size_y, size_y + size_z)
        corner = slice(size_y + size_z, size_y + size_z + 1)
        read = value[side] + fx * slope[side]
        read_c = value[corner] + fx * slope[corner]
        h_w = jnp.sum(read * w_z, axis=0, keepdims=True) + read_c * wz_top
        h_d = jnp.sum(read * d_z, axis=0, keepdims=True) + read_c * dz_top
        h_x = jnp.sum(slope[side] * w_z, axis=0, keepdims=True) + slope[corner] * wz_top
        record = (slots[:, span] + 1).astype(F32)
        vals_s[:, span] = jnp.concatenate(
            [grad_z + wy_top * h_d, grad_y + dy_top * h_w, grad_x + wy_top * h_x, record] * 2, axis=0)

    early = chunks // 4
    for j in range(early):
        main_chunk(j)
    pl.semaphore_wait(barrier, devices - 1)
    below_z = lax.rem(gz + count_z - 1, count_z)
    below_y = lax.rem(gy + count_y - 1, count_y)
    halos = []
    for i, (source, target, device) in enumerate((
        (grid_ref.at[0], halo_z, (below_z, gy)),
        (row_s, halo_y, (gz, below_y)),
        (corner_s, halo_c, (below_z, below_y)),
    )):
        halos.append(pltpu.make_async_remote_copy(
            src_ref=source, dst_ref=target, send_sem=halo_send.at[i], recv_sem=halo_recv.at[i],
            device_id=device, device_id_type=MESH,
        ))
        halos[-1].start()

    for j in range(early, chunks):
        main_chunk(j)
    for copy in halos:
        copy.wait()
    ghost = with_diff(jnp.concatenate(
        [halo_z[...], halo_y[...], jnp.broadcast_to(halo_c[...], (8, size_x))], axis=0))
    for j in range(chunks):
        halo_chunk(j, ghost)

    def pack_group(g, carry):
        wide = 4 * group
        whose = lax.shift_right_logical(iota((wide, rows), 0), 2) + g * group
        values = jnp.concatenate([vals_s[...]] * (wide // 8), axis=0)
        high, low = split(jnp.where(whose == owner, values, 0.0))
        packed = dot_nt(high, rank_s[...]) + dot_nt(low, rank_s[...])
        for d in range(group):
            send_s[g * group + d] = packed[4 * d:4 * d + 4]
        return carry

    over(groups, pack_group, 0)

    def exchange(source, target, device):
        return pltpu.make_async_remote_copy(
            src_ref=source, dst_ref=target, send_sem=all_send, recv_sem=all_recv,
            device_id=device, device_id_type=MESH,
        )

    def post(to_z, to_y):
        other = to_z * count_y + to_y
        exchange(send_s.at[other], recv_s.at[me], (to_z, to_y)).start()

    each_other(post)
    recv_s[me] = send_s[me]
    others = pl.ds(0, devices - 1)
    exchange(send_s.at[others], recv_s.at[others], (below_z, below_y)).wait()

    highs = rows // LANES

    def add_group(g, total):
        block = jnp.concatenate([recv_s[g * group + d] for d in range(group)], axis=1)
        record = block[3:4].astype(jnp.int32) - 1
        high_at = lax.shift_right_arithmetic(record, 7)
        low_at = lax.bitwise_and(record, LANES - 1)
        width = block.shape[1]
        low_hot = hot(iota((LANES, width), 0) == low_at)
        values = jnp.concatenate([block] * highs, axis=0)
        which = lax.shift_right_logical(iota((4 * highs, width), 0), 2)
        both = jnp.concatenate(split(jnp.where(which == high_at, values, 0.0)), axis=0)
        added = dot_nt(both, low_hot)
        return total + added[:4 * highs] + added[4 * highs:]

    total = over(groups, add_group, jnp.zeros((4 * highs, LANES), F32))
    for h in range(highs):
        out[:, h * LANES:(h + 1) * LANES] = total[4 * h:4 * h + 3]


def body(grid_grad, cells, offsets, owners, slots):
    size_z, size_y, size_x = grid_grad.shape
    rows = cells.shape[1]
    devices = lax.axis_size("gz") * lax.axis_size("gy")
    vmem = pl.BlockSpec(memory_space=pltpu.VMEM)
    hbm = pl.BlockSpec(memory_space=pltpu.HBM)
    return pl.pallas_call(
        kernel,
        out_shape=jax.ShapeDtypeStruct((3, rows), F32),
        in_specs=[hbm] * 5,
        out_specs=vmem,
        scratch_shapes=[
            pltpu.VMEM((3, rows), jnp.int32),
            pltpu.VMEM((3, rows), jnp.int32),
            pltpu.VMEM((1, rows), jnp.int32),
            pltpu.VMEM((1, rows), jnp.int32),
            pltpu.VMEM((size_z, size_y, size_x), F32),
            pltpu.VMEM((size_z, size_x), F32),
            pltpu.VMEM((1, size_x), F32),
            pltpu.VMEM((size_y, size_x), F32),
            pltpu.VMEM((size_z, size_x), F32),
            pltpu.VMEM((1, size_x), F32),
            pltpu.VMEM((4 * size_z * size_y, size_x), BF),
            pltpu.VMEM((size_x, rows), BF),
            pltpu.VMEM((4, size_y, rows), F32),
            pltpu.VMEM((LANES, rows), BF),
            pltpu.VMEM((8, rows), F32),
            pltpu.VMEM((devices, 4, LANES), F32),
            pltpu.VMEM((devices, 4, LANES), F32),
            pltpu.SemaphoreType.DMA((5,)),
            pltpu.SemaphoreType.DMA((3,)),
            pltpu.SemaphoreType.DMA((3,)),
            pltpu.SemaphoreType.DMA,
            pltpu.SemaphoreType.DMA,
        ],
        compiler_params=pltpu.CompilerParams(collective_id=0, has_side_effects=True, vmem_limit_bytes=60 * 1024 * 1024),
        name="cic",
    )(grid_grad, cells, offsets, owners.reshape(1, rows), slots.reshape(1, rows))


def solution(mesh):
    placed = (
        P("gz", "gy", None),
        P(None, ("gz", "gy")),
        P(None, ("gz", "gy")),
        P(("gz", "gy"), None),
        P(("gz", "gy")),
    )
    return jax.shard_map(
        body, mesh=mesh, in_specs=placed, out_specs=P(None, ("gz", "gy")), check_vma=False
    )
```

```python
import jax
import jax.numpy as jnp
from jax import lax
from jax.experimental import pallas as pl
from jax.experimental.pallas import tpu as pltpu
from jax.sharding import PartitionSpec as P

MESH = pl.DeviceIdType.MESH
BF = jnp.bfloat16
F32 = jnp.float32
LANES = 128


def iota(shape, axis):
    return lax.broadcasted_iota(jnp.int32, shape, axis)


def hot(mask):
    return jnp.where(mask, 1.0, 0.0).astype(BF)


def split(value):
    high = value.astype(BF)
    low = (value - high.astype(F32)).astype(BF)
    return high, low


def dot_nn(a, b):
    return lax.dot_general(a, b, (((1,), (0,)), ((), ())), preferred_element_type=F32)


def dot_nt(a, b):
    return lax.dot_general(a, b, (((1,), (1,)), ((), ())), preferred_element_type=F32)


def with_diff(rows):
    size_x = rows.shape[1]
    diff = pltpu.roll(rows, size_x - 1, 1) - rows
    return jnp.concatenate([*split(rows), *split(diff)], axis=0)


def over(count, step, carry):
    if count == 1:
        return step(0, carry)
    return lax.fori_loop(0, count, step, carry)


def kernel(
    grid_ref, cells_ref, offsets_ref, owners_ref, slots_ref, recv_s,
    cells, offsets, owners, slots, grid_v, row_s, corner_s, halo_z, halo_y, halo_c, mesh_s, hot_s, acc_s, rank_s, vals_s,
    send_s, load_sem, own_sem, halo_send, halo_recv, all_send, all_recv,
):
    count_z, count_y = lax.axis_size("gz"), lax.axis_size("gy")
    devices = count_z * count_y
    gz, gy = lax.axis_index("gz"), lax.axis_index("gy")
    me = gz * count_y + gy
    size_z, size_y, size_x = grid_ref.shape
    rows = cells.shape[1]
    chunk = min(256, rows)
    chunks = rows // chunk
    group = min(32, devices)
    groups = devices // group
    slab = size_z * size_y

    loads = []
    for i, (source, target) in enumerate((
        (owners_ref, owners), (grid_ref, grid_v), (cells_ref, cells),
        (offsets_ref, offsets), (slots_ref, slots),
    )):
        loads.append(pltpu.make_async_copy(source, target, load_sem.at[i]))
        loads[-1].start()
    barrier = pltpu.get_barrier_semaphore()

    def each_other(act):
        few = devices <= 64

        def along_y(to_z, first):
            def step(shift, carry):
                act(to_z, lax.rem(gy + shift, count_y))
                return carry
            lax.fori_loop(first, count_y, step, 0, unroll=few)

        def step_z(shift, carry):
            along_y(lax.rem(gz + shift, count_z), 0)
            return carry
        lax.fori_loop(1, count_z, step_z, 0, unroll=few)
        along_y(gz, 1)

    def greet(to_z, to_y):
        pl.semaphore_signal(barrier, inc=1, device_id=(to_z, to_y), device_id_type=MESH)

    each_other(greet)

    loads[0].wait()
    owner = owners[...]
    before = hot(iota((chunk, chunk), 0) < iota((chunk, chunk), 1))

    def rank_group(g, ranks):
        mine = jnp.where(iota((group, rows), 0) + g * group == owner, 1.0, 0.0)
        pieces = [mine[:, c * chunk:(c + 1) * chunk] for c in range(chunks)]
        inside = dot_nn(jnp.concatenate(pieces, axis=0).astype(BF), before)
        start = jnp.zeros((group, 1), F32)
        found = []
        for c in range(chunks):
            where = inside[c * group:(c + 1) * group] + start
            found.append(jnp.sum(pieces[c] * where, axis=0, keepdims=True))
            start = start + jnp.sum(pieces[c], axis=1, keepdims=True)
        return ranks + jnp.concatenate(found, axis=1)

    ranks = over(groups, rank_group, jnp.zeros((1, rows), F32))
    rank_s[...] = hot(iota((LANES, rows), 0) == ranks.astype(jnp.int32))

    loads[1].wait()
    row_s[...] = grid_v[:, 0, :]
    corner_s[...] = grid_v[0, 0:1, :]
    mesh_s[...] = with_diff(grid_v[...].reshape(slab, size_x))

    for copy in loads[2:]:
        copy.wait()

    def place(j):
        span = pl.ds(j * chunk, chunk)
        cell = cells[:, span]
        frac = (offsets[:, span].astype(F32) + 0.5) / 1024.0
        return (span, cell[0:1] - gz * size_z, cell[1:2] - gy * size_y, cell[2:3],
                frac[0:1], frac[1:2], frac[2:3])

    def main_chunk(j):
        span, cz, cy, cx, fz, fy, fx = place(j)
        onehot = hot(iota((size_x, chunk), 0) == cx)
        hot_s[:, span] = onehot
        prod = dot_nn(mesh_s[...], onehot)
        cz, fz = jnp.broadcast_to(cz, (8, chunk)), jnp.broadcast_to(fz, (8, chunk))
        gz0 = 1.0 - fz
        tiles = size_y // 8
        total = [[jnp.zeros((8, chunk), F32) for _ in range(tiles)] for _ in range(4)]
        for z in range(size_z):
            lower, upper = cz == z, cz == z - 1
            weight = jnp.where(lower, gz0, jnp.where(upper, fz, 0.0))
            diff = jnp.where(lower, -1.0, jnp.where(upper, 1.0, 0.0))
            for t in range(tiles):
                first = z * size_y + 8 * t
                at = [prod[q * slab + first:q * slab + first + 8] for q in range(4)]
                value, slope = at[0] + at[1], at[2] + at[3]
                total[0][t] += weight * value
                total[1][t] += diff * value
                total[2][t] += weight * slope
                total[3][t] += diff * slope
        for q in range(4):
            acc_s[q, :, span] = jnp.concatenate(total[q], axis=0)

    part = size_y + size_z + 8

    def halo_chunk(j, ghost):
        span, cz, cy, cx, fz, fy, fx = place(j)
        prod = dot_nn(ghost, hot_s[:, span])
        value = prod[:part] + prod[part:2 * part]
        slope = prod[2 * part:3 * part] + prod[3 * part:]
        top_z, top_y = cz == size_z - 1, cy == size_y - 1
        wz_top, dz_top = jnp.where(top_z, fz, 0.0), jnp.where(top_z, 1.0, 0.0)
        wy_top, dy_top = jnp.where(top_y, fy, 0.0), jnp.where(top_y, 1.0, 0.0)
        a_w = acc_s[0, :, span] + wz_top * value[:size_y]
        a_d = acc_s[1, :, span] + dz_top * value[:size_y]
        b_w = acc_s[2, :, span] + wz_top * slope[:size_y]
        b_d = acc_s[3, :, span] + dz_top * slope[:size_y]
        place_y = iota((size_y, chunk), 0)
        lower, upper = place_y == cy, place_y == cy + 1
        w_y = jnp.where(lower, 1.0 - fy, jnp.where(upper, fy, 0.0))
        d_y = jnp.where(lower, -1.0, jnp.where(upper, 1.0, 0.0))
        grad_z = jnp.sum((a_d + fx * b_d) * w_y, axis=0, keepdims=True)
        grad_y = jnp.sum((a_w + fx * b_w) * d_y, axis=0, keepdims=True)
        grad_x = jnp.sum(b_w * w_y, axis=0, keepdims=True)
        place_z = iota((size_z, chunk), 0)
        lower, upper = place_z == cz, place_z == cz + 1
        w_z = jnp.where(lower, 1.0 - fz, jnp.where(upper, fz, 0.0))
        d_z = jnp.where(lower, -1.0, jnp.where(upper, 1.0, 0.0))
        side = slice(size_y, size_y + size_z)
        corner = slice(size_y + size_z, size_y + size_z + 1)
        read = value[side] + fx * slope[side]
        read_c = value[corner] + fx * slope[corner]
        h_w = jnp.sum(read * w_z, axis=0, keepdims=True) + read_c * wz_top
        h_d = jnp.sum(read * d_z, axis=0, keepdims=True) + read_c * dz_top
        h_x = jnp.sum(slope[side] * w_z, axis=0, keepdims=True) + slope[corner] * wz_top
        record = (slots[:, span] + 1).astype(F32)
        vals_s[:, span] = jnp.concatenate(
            [grad_z + wy_top * h_d, grad_y + dy_top * h_w, grad_x + wy_top * h_x, record] * 2, axis=0)

    early = chunks // 4
    for j in range(early):
        main_chunk(j)
    pl.semaphore_wait(barrier, devices - 1)
    below_z = lax.rem(gz + count_z - 1, count_z)
    below_y = lax.rem(gy + count_y - 1, count_y)
    halos = []
    for i, (source, target, device) in enumerate((
        (corner_s, halo_c, (below_z, below_y)),
        (grid_ref.at[0], halo_z, (below_z, gy)),
        (row_s, halo_y, (gz, below_y)),
    )):
        halos.append(pltpu.make_async_remote_copy(
            src_ref=source, dst_ref=target, send_sem=halo_send.at[i], recv_sem=halo_recv.at[i],
            device_id=device, device_id_type=MESH,
        ))
        halos[-1].start()

    for j in range(early, chunks):
        main_chunk(j)
    for copy in halos:
        copy.wait()
    ghost = with_diff(jnp.concatenate(
        [halo_z[...], halo_y[...], jnp.broadcast_to(halo_c[...], (8, size_x))], axis=0))
    for j in range(chunks):
        halo_chunk(j, ghost)

    def pack_group(g, carry):
        wide = 4 * group
        whose = lax.shift_right_logical(iota((wide, rows), 0), 2) + g * group
        values = jnp.concatenate([vals_s[...]] * (wide // 8), axis=0)
        high, low = split(jnp.where(whose == owner, values, 0.0))
        packed = dot_nt(high, rank_s[...]) + dot_nt(low, rank_s[...])
        for d in range(group):
            send_s[g * group + d] = packed[4 * d:4 * d + 4]
        return carry

    over(groups, pack_group, 0)

    def exchange(source, target, device):
        return pltpu.make_async_remote_copy(
            src_ref=source, dst_ref=target, send_sem=all_send, recv_sem=all_recv,
            device_id=device, device_id_type=MESH,
        )

    own = pltpu.make_async_copy(send_s.at[me], recv_s.at[me], own_sem)

    def post(to_z, to_y):
        other = to_z * count_y + to_y
        exchange(send_s.at[other], recv_s.at[me], (to_z, to_y)).start()

    each_other(post)
    own.start()
    own.wait()
    others = pl.ds(0, devices - 1)
    exchange(send_s.at[others], recv_s.at[others], (below_z, below_y)).wait()


def scatter(recv_s, out):
    devices, rows = recv_s.shape[0], out.shape[1]
    group = min(32, devices)
    groups = devices // group
    highs = rows // LANES

    def add_group(g, total):
        block = jnp.concatenate([recv_s[g * group + d] for d in range(group)], axis=1)
        record = block[3:4].astype(jnp.int32) - 1
        high_at = lax.shift_right_arithmetic(record, 7)
        low_at = lax.bitwise_and(record, LANES - 1)
        width = block.shape[1]
        low_hot = hot(iota((LANES, width), 0) == low_at)
        values = jnp.concatenate([block] * highs, axis=0)
        which = lax.shift_right_logical(iota((4 * highs, width), 0), 2)
        both = jnp.concatenate(split(jnp.where(which == high_at, values, 0.0)), axis=0)
        added = dot_nt(both, low_hot)
        return total + added[:4 * highs] + added[4 * highs:]

    total = over(groups, add_group, jnp.zeros((4 * highs, LANES), F32))
    for h in range(highs):
        out[:, h * LANES:(h + 1) * LANES] = total[4 * h:4 * h + 3]


def body(grid_grad, cells, offsets, owners, slots):
    size_z, size_y, size_x = grid_grad.shape
    rows = cells.shape[1]
    devices = lax.axis_size("gz") * lax.axis_size("gy")
    vmem = pl.BlockSpec(memory_space=pltpu.VMEM)
    hbm = pl.BlockSpec(memory_space=pltpu.HBM)
    received = pl.pallas_call(
        kernel,
        out_shape=jax.ShapeDtypeStruct((devices, 4, LANES), F32),
        in_specs=[hbm] * 5,
        out_specs=hbm,
        scratch_shapes=[
            pltpu.VMEM((3, rows), jnp.int32),
            pltpu.VMEM((3, rows), jnp.int32),
            pltpu.VMEM((1, rows), jnp.int32),
            pltpu.VMEM((1, rows), jnp.int32),
            pltpu.VMEM((size_z, size_y, size_x), F32),
            pltpu.VMEM((size_z, size_x), F32),
            pltpu.VMEM((1, size_x), F32),
            pltpu.VMEM((size_y, size_x), F32),
            pltpu.VMEM((size_z, size_x), F32),
            pltpu.VMEM((1, size_x), F32),
            pltpu.VMEM((4 * size_z * size_y, size_x), BF),
            pltpu.VMEM((size_x, rows), BF),
            pltpu.VMEM((4, size_y, rows), F32),
            pltpu.VMEM((LANES, rows), BF),
            pltpu.VMEM((8, rows), F32),
            pltpu.VMEM((devices, 4, LANES), F32),
            pltpu.SemaphoreType.DMA((5,)),
            pltpu.SemaphoreType.DMA,
            pltpu.SemaphoreType.DMA((3,)),
            pltpu.SemaphoreType.DMA((3,)),
            pltpu.SemaphoreType.DMA,
            pltpu.SemaphoreType.DMA,
        ],
        compiler_params=pltpu.CompilerParams(collective_id=0, has_side_effects=True, vmem_limit_bytes=60 * 1024 * 1024),
        name="cic",
    )(grid_grad, cells, offsets, owners.reshape(1, rows), slots.reshape(1, rows))
    return pl.pallas_call(
        scatter,
        out_shape=jax.ShapeDtypeStruct((3, rows), F32),
        in_specs=[vmem],
        out_specs=vmem,
        compiler_params=pltpu.CompilerParams(vmem_limit_bytes=60 * 1024 * 1024),
        name="scatter",
    )(received)


def solution(mesh):
    placed = (
        P("gz", "gy", None),
        P(None, ("gz", "gy")),
        P(None, ("gz", "gy")),
        P(("gz", "gy"), None),
        P(("gz", "gy")),
    )
    return jax.shard_map(
        body, mesh=mesh, in_specs=placed, out_specs=P(None, ("gz", "gy")), check_vma=False
    )
```
